32 devices in a mesh: tok: 16 (over z, y, core), lay: 2 (over x).
Axes of the slice: x: 2, y: 2, z: 4, core: 2. Of those that a mesh axis runs over, the one named last changes fastest.
Arguments:
- first_acts: bfloat16 [2, 4096, 5120], P('lay', 'tok'), may hold values from -40 to 40
- second_acts: bfloat16 [2, 4096, 5120], P('lay', 'tok'), may hold values from -40 to 40
Outputs:
- whitening: float32 [2, 2, 40, 128, 128], P(None, 'lay')
- similarity: float32 [2, 2, 40], P('lay')
The draws below stay inside these ranges and needn't reach their ends.
All inputs are finite; a program needn't handle non-finite values.
Results may differ from the reference program's by a relative error of at most 0.0003.
Values may be sent and summed in bfloat16 or wider, within the bound.
No kernel may reach another device: no remote copies, remote signals or barrier semaphores. Data moves between devices by JAX's collectives and lax.ppermute only.
A program may use at most 128 MiB of HBM per device.

```python
import math
import jax
import jax.numpy as jnp
from jax import lax

HEADS = 40
HEAD_DIM = 128
D = 5120
ITERS = 6
LAYERS = 2
TOKENS = 4096


def residual_layers(key):
    row_position = jnp.arange(TOKENS, dtype=jnp.float32) / TOKENS
    row_jitter = jax.random.uniform(jax.random.fold_in(key, 11), (TOKENS,), jnp.float32, -0.35, 0.35)
    row_scale = jnp.exp(math.log(3.0) * row_position + row_jitter)
    mixing = jnp.eye(HEAD_DIM, dtype=jnp.float32) + 0.8 / math.sqrt(HEAD_DIM) * jax.random.normal(jax.random.fold_in(key, 12), (HEADS, HEAD_DIM, HEAD_DIM), jnp.float32)
    stream = jnp.zeros((TOKENS, D), jnp.float32)
    first_list = []
    second_list = []
    for layer_idx in range(LAYERS):
        layer_key = jax.random.fold_in(key, 1000 + layer_idx)
        update = jax.random.normal(jax.random.fold_in(layer_key, 1), (TOKENS, D), jnp.float32)
        noise_part = jax.random.normal(jax.random.fold_in(layer_key, 3), (TOKENS, D), jnp.float32)
        chan_low = 0.3
        chan_high = 3.0
        stream = 0.8 * stream + 0.6 * update
        mixed_stream = jnp.einsum('thi,hij->thj', stream.reshape(TOKENS, HEADS, HEAD_DIM), mixing, precision=lax.Precision.HIGHEST).reshape(TOKENS, D)
        chan_first = jnp.exp(jax.random.uniform(jax.random.fold_in(layer_key, 4), (D,), jnp.float32, math.log(chan_low), math.log(chan_high)))
        chan_second = chan_first * jnp.exp(jax.random.uniform(jax.random.fold_in(layer_key, 5), (D,), jnp.float32, -0.35, 0.35))
        offset_first = 0.8 * jax.random.normal(jax.random.fold_in(layer_key, 6), (D,), jnp.float32)
        offset_second = offset_first + 0.3 * jax.random.normal(jax.random.fold_in(layer_key, 7), (D,), jnp.float32)
        first_layer = row_scale[:, None] * (chan_first * mixed_stream + offset_first)
        second_layer = row_scale[:, None] * (chan_second * (0.75 * mixed_stream + 0.66 * noise_part) + offset_second)
        first_list.append(jnp.clip(first_layer, -40.0, 40.0))
        second_list.append(jnp.clip(second_layer, -40.0, 40.0))
    return (jnp.stack(first_list), jnp.stack(second_list))


def draw_first_acts(key, part):
    return residual_layers(key)[0].astype(jnp.bfloat16)


def draw_second_acts(key, part):
    return residual_layers(key)[1].astype(jnp.bfloat16)


def setup_inputs(seed: int = 0) -> dict:
    arg_keys = jax.random.split(jax.random.key(seed), 3)
    return {
        "first_acts": draw_first_acts(jax.random.fold_in(arg_keys[2], 71), 0),
        "second_acts": draw_second_acts(jax.random.fold_in(arg_keys[2], 71), 0),
    }


ridge_weight = 0.05
top_precision = lax.Precision.HIGHEST

def newton_whiten(matrices):
    unit_matrix = jnp.eye(HEAD_DIM, dtype=jnp.float32)
    scale_norm = jnp.sqrt(lax.optimization_barrier(jnp.sum(matrices * matrices, axis=(-2, -1), keepdims=True)))
    square_iter = matrices / scale_norm
    inverse_iter = jnp.broadcast_to(unit_matrix, matrices.shape)
    for sweep_index in range(ITERS):
        factor_iter = 1.5 * unit_matrix - 0.5 * jnp.matmul(inverse_iter, square_iter, precision=top_precision)
        square_iter = jnp.matmul(square_iter, factor_iter, precision=top_precision)
        inverse_iter = jnp.matmul(factor_iter, inverse_iter, precision=top_precision)
    return inverse_iter / jnp.sqrt(scale_norm)

def covariance(gram_total, col_sums, token_total):
    unit_matrix = jnp.eye(HEAD_DIM, dtype=jnp.float32)
    column_mean = col_sums / token_total
    return gram_total / token_total - column_mean[..., :, None] * column_mean[..., None, :] + ridge_weight * unit_matrix

def head_view(act_block):
    return act_block.astype(jnp.float32).reshape(TOKENS, HEADS, HEAD_DIM)

def reference(first_acts, second_acts):
    gram_list = []
    sums_list = []
    for checkpoint in (first_acts, second_acts):
        for layer_idx in range(LAYERS):
            viewed = head_view(checkpoint[layer_idx])
            gram_list.append(jnp.einsum('thi,thj->hij', viewed, viewed, precision=top_precision))
            sums_list.append(lax.optimization_barrier(jnp.sum(viewed, axis=0)))
    gram_total = jnp.stack(gram_list).reshape(2, LAYERS, HEADS, HEAD_DIM, HEAD_DIM)
    col_sums = jnp.stack(sums_list).reshape(2, LAYERS, HEADS, HEAD_DIM)
    whitening = newton_whiten(covariance(gram_total, col_sums, TOKENS))
    column_mean = col_sums / TOKENS
    rows_out = []
    for first_idx in range(LAYERS):
        view_first = head_view(first_acts[first_idx])
        row_items = []
        for second_idx in range(LAYERS):
            view_second = head_view(second_acts[second_idx])
            cross_cov = jnp.einsum('thi,thj->hij', view_first, view_second, precision=top_precision) / TOKENS
            cross_cov = cross_cov - column_mean[0, first_idx][:, :, None] * column_mean[1, second_idx][:, None, :]
            left_product = jnp.matmul(whitening[0, first_idx], cross_cov, precision=top_precision)
            whitened = jnp.matmul(left_product, whitening[1, second_idx], precision=top_precision)
            row_items.append(lax.optimization_barrier(jnp.sum(whitened * whitened, axis=(-2, -1))) / HEAD_DIM)
        rows_out.append(jnp.stack(row_items))
    return (whitening, jnp.stack(rows_out))
```

```python
import functools

import jax
import jax.numpy as jnp
from jax import lax
from jax.experimental import pallas as pl
from jax.experimental.pallas import tpu as pltpu
from jax.sharding import PartitionSpec as P

HEAD_DIM = 128
HALF = HEAD_DIM // 2
ITERS = 6
GROUPS = 8
RIDGE = 0.05
TOP = lax.Precision.HIGHEST
F32 = jnp.float32


def iotas(rows):
    row = lax.broadcasted_iota(jnp.int32, (rows, HEAD_DIM), 0)
    lane = lax.broadcasted_iota(jnp.int32, (rows, HEAD_DIM), 1)
    return row, lane


def pack_sym(mat):
    row, lane = iotas(HALF)
    low = mat[HALF:]
    packed = jnp.where(row <= lane, mat[:HALF], pltpu.roll(low, HALF, 1))
    diag = jnp.sum(jnp.where(lane - HALF == row, low, 0.0), axis=0, keepdims=True)
    return packed, diag


def unpack_sym(packed, diag):
    row, lane = iotas(HALF)
    square = jnp.concatenate([packed, packed], axis=0).T
    turned = square[:HALF]
    top = jnp.where(row <= lane, packed, turned)
    corner = jnp.where(row > lane - HALF, pltpu.roll(packed, HALF, 1), turned)
    corner = jnp.where(row == lane - HALF, diag, corner)
    bottom = jnp.where(lane < HALF, square[HALF:], corner)
    return jnp.concatenate([top, bottom], axis=0)


def outer(left_row, right_row):
    column = jnp.broadcast_to(left_row, (HEAD_DIM, HEAD_DIM)).T
    return column * right_row


def mm(a, b):
    return jnp.dot(a, b, precision=TOP, preferred_element_type=F32)


def contract_tokens(a, b):
    return lax.dot_general(a, b, (((0,), (0,)), ((), ())), preferred_element_type=F32)


def pack_kernel(per, cut, idx, x1o, x2k, x2o, o1, oak, obk, oao, obo):
    o1[...] = x1o[...]
    oak[...] = x2k[:, :cut]
    obk[...] = x2k[:, cut:]
    oao[...] = x2o[:, :cut]
    obo[...] = x2o[:, cut:]


def gram_kernel(per, first_part, idx, x1, x1r, x2, x2ra, x2rb, s1, k1, s2, k2, sa, ka, sb, kb):
    slot = pl.program_id(0)
    rows = per * HALF
    packs = [[], []]
    sums = [[], []]
    diags = [[], []]
    cross = []
    for q in range(per):
        cols = slice(q * HEAD_DIM, (q + 1) * HEAD_DIM)
        if q < first_part:
            r2 = x2ra[:, cols]
        else:
            r2 = x2rb[:, (q - first_part) * HEAD_DIM : (q - first_part + 1) * HEAD_DIM]
        mine = jnp.concatenate([x1[:, cols], x2[:, cols]], axis=1)
        theirs = jnp.concatenate([x1r[:, cols], r2], axis=1)
        both = jnp.concatenate([mine, theirs], axis=0)
        g = contract_tokens(both, both)
        total = jnp.sum(both.astype(F32), axis=0, keepdims=True)
        for c in range(2):
            part = slice(c * HEAD_DIM, (c + 1) * HEAD_DIM)
            packed, diag = pack_sym(g[part, part])
            packs[c].append(packed)
            diags[c].append(diag)
            sums[c].append(total[:, part])
        cross.append(g[:HEAD_DIM, HEAD_DIM:])

    def write(ref, c):
        for q in range(per):
            ref[0, q * HALF : (q + 1) * HALF, :] = packs[c][q]
        tail = jnp.zeros((ref.shape[1] - rows - 2 * per, HEAD_DIM), F32)
        ref[0, rows:, :] = jnp.concatenate(sums[c] + diags[c] + [tail], axis=0)

    def write_cross(ref, lo, hi):
        for q in range(lo, hi):
            ref[0, q - lo] = cross[q]

    @pl.when(slot >= 2)
    def _():
        write(s1, 0)
        write_cross(sa, 0, first_part)

    @pl.when(slot < 2)
    def _():
        write(k1, 0)
        write_cross(ka, 0, first_part)

    @pl.when(slot % 2 == 1)
    def _():
        write(s2, 1)
        write_cross(sb, first_part, per)

    @pl.when(slot % 2 == 0)
    def _():
        write(k2, 1)
        write_cross(kb, first_part, per)


def cross_kernel(lo, count, by_first, idx, x1, x1r, xm, xt, send, keep):
    slot = pl.program_id(0)
    out = []
    for q in range(count):
        left = slice((lo + q) * HEAD_DIM, (lo + q + 1) * HEAD_DIM)
        right = slice(q * HEAD_DIM, (q + 1) * HEAD_DIM)
        a = jnp.concatenate([x1[:, left], x1r[:, left]], axis=0)
        b = jnp.concatenate([xm[:, right], xt[:, right]], axis=0)
        out.append(contract_tokens(a, b))
    moves = slot >= 2 if by_first else slot % 2 == 1

    @pl.when(moves)
    def _():
        for q in range(count):
            send[0, q] = out[q]

    @pl.when(jnp.logical_not(moves))
    def _():
        for q in range(count):
            keep[0, q] = out[q]


def newton_kernel(per, tokens, keep, recv, out):
    rows = per * HALF
    total = keep[...] + recv[...]
    row = lax.broadcasted_iota(jnp.int32, (HEAD_DIM, HEAD_DIM), 0)
    lane = lax.broadcasted_iota(jnp.int32, (HEAD_DIM, HEAD_DIM), 1)
    eye = jnp.where(row == lane, 1.0, 0.0).astype(F32)
    ys, zs, scales, means = [], [], [], []
    for q in range(per):
        gram = unpack_sym(
            total[q * HALF : (q + 1) * HALF], total[rows + per + q : rows + per + q + 1]
        )
        mean = total[rows + q : rows + q + 1] / tokens
        cov = gram / tokens - outer(mean, mean) + RIDGE * eye
        scale = jnp.sqrt(jnp.sum(cov * cov, keepdims=True))
        y = cov / scale
        ys.append(y)
        scales.append(scale)
        means.append(mean)
    fs = [1.5 * eye - 0.5 * y for y in ys]
    ys = [mm(y, f) for y, f in zip(ys, fs)]
    zs = fs
    for sweep in range(1, ITERS):
        fs = [1.5 * eye - 0.5 * mm(z, y) for z, y in zip(zs, ys)]
        if sweep < ITERS - 1:
            ys = [mm(y, f) for y, f in zip(ys, fs)]
        zs = [mm(f, z) for f, z in zip(fs, zs)]
    diags = []
    for q in range(per):
        packed, diag = pack_sym(zs[q] / jnp.sqrt(scales[q]))
        out[q * HALF : (q + 1) * HALF, :] = packed
        diags.append(diag)
    tail = jnp.zeros((out.shape[0] - rows - 2 * per, HEAD_DIM), F32)
    out[rows:, :] = jnp.concatenate(means + diags + [tail], axis=0)


def head_of(pack, per, q):
    rows = per * HALF
    mat = unpack_sym(pack[q * HALF : (q + 1) * HALF], pack[rows + per + q : rows + per + q + 1])
    return mat, pack[rows + q : rows + q + 1]


def similar_kernel(per, first_part, tokens, idx, w1, w2, ca, cb, out):
    row, lane = iotas(8)
    tile = jnp.zeros((8, HEAD_DIM), F32)
    for q in range(per):
        left, mean_left = head_of(w1, per, q)
        right, mean_right = head_of(w2, per, q)
        if q < first_part:
            cross = ca[0, q] + ca[1, q]
        else:
            cross = cb[0, q - first_part] + cb[1, q - first_part]
        cross = cross / tokens - outer(mean_left, mean_right)
        white = mm(mm(left, cross), right)
        value = jnp.sum(white * white, keepdims=True) / HEAD_DIM
        mine = idx[0] == (0 if q < first_part else 1)
        place = (row == idx[1]) & (lane == idx[2] + q) & mine
        tile = jnp.where(place, value, tile)
    out[...] = tile


def spread_kernel(per, count, fresh, idx, *refs):
    sources = refs[:count]
    out, buf = refs[-2], refs[-1]
    step = pl.program_id(0)
    for i, source in enumerate(sources):

        @pl.when(step == i)
        def _(source=source):
            buf[...] = source[...]

    for q in range(per):
        mat, _ = head_of(buf, per, q)
        out[0, 0, q] = mat


def local(first_acts, second_acts):
    n_tok = lax.axis_size("tok")
    n_lay = lax.axis_size("lay")
    layers, rows, width = first_acts.shape
    heads = width // HEAD_DIM
    bits = n_tok.bit_length() - 1
    assert layers == 1 and n_lay == 2
    assert n_tok == 1 << bits and bits >= 4 and heads % GROUPS == 0
    per = heads // GROUPS
    first_part = (per + 1) // 2
    rest = per - first_part
    block = per * HEAD_DIM
    cut = first_part * HEAD_DIM
    tokens = float(rows * n_tok)
    pack_rows = -(-(per * HALF + 2 * per) // 8) * 8

    tok = lax.axis_index("tok")
    lay = lax.axis_index("lay")
    bit = [(tok >> b) & 1 for b in range(bits)]

    def swap(x, b):
        return lax.ppermute(x, "tok", [(i, i ^ (1 << b)) for i in range(n_tok)])

    def one_way(x, b, target):
        pairs = [(i, i ^ (1 << b)) for i in range(n_tok) if (i >> b) & 1 != target]
        return lax.ppermute(x, "tok", pairs)

    def over_lay(x, flip):
        pairs = [(t * 2 + l, (t ^ flip) * 2 + 1 - l) for t in range(n_tok) for l in range(2)]
        return lax.ppermute(x, ("tok", "lay"), pairs)

    x1 = first_acts[0]
    x2 = second_acts[0]
    quarter = GROUPS // 2
    group = bit[0] * quarter + bit[1] * 2 + bit[2]
    idx = jnp.stack([bit[0], bit[1], bit[2]]).astype(jnp.int32)

    own = lambda i, s: (0, s[0] * quarter + i)
    oth = lambda i, s: (0, (1 - s[0]) * quarter + i)
    plain = lambda i, s: (0, i)
    bf = first_acts.dtype
    narrow = rest * HEAD_DIM
    x1o, x2ak, x2bk, x2ao, x2bo = pl.pallas_call(
        functools.partial(pack_kernel, per, cut),
        grid_spec=pltpu.PrefetchScalarGridSpec(
            num_scalar_prefetch=1,
            grid=(quarter,),
            in_specs=[
                pl.BlockSpec((rows, block), oth),
                pl.BlockSpec((rows, block), own),
                pl.BlockSpec((rows, block), oth),
            ],
            out_specs=[
                pl.BlockSpec((rows, block), plain),
                pl.BlockSpec((rows, cut), plain),
                pl.BlockSpec((rows, narrow), plain),
                pl.BlockSpec((rows, cut), plain),
                pl.BlockSpec((rows, narrow), plain),
            ],
        ),
        out_shape=[
            jax.ShapeDtypeStruct((rows, quarter * w), bf) for w in (block, cut, narrow, cut, narrow)
        ],
        name="pack",
    )(idx, x1, x2, x2)

    x1r = swap(x1o, 0)
    x2ra = swap(x2ao, 0)
    x2rb = swap(x2bo, 0)
    xam = over_lay(x2ak, 0)
    xat = over_lay(x2ao, 1)
    xbm = over_lay(x2bk, 0)
    xbt = over_lay(x2bo, 1)

    def mine(i, s):
        return (0, s[0] * quarter + (s[1] ^ (i // 2)) * 2 + (s[2] ^ (i % 2)))

    def half(i, s):
        return (0, (s[1] ^ (i // 2)) * 2 + (s[2] ^ (i % 2)))

    send_a = lambda i, s: (jnp.maximum(i - 2, 0), 0, 0)
    keep_a = lambda i, s: (jnp.minimum(i, 1), 0, 0)
    send_b = lambda i, s: (i // 3, 0, 0)
    keep_b = lambda i, s: (i // 2, 0, 0)
    four = lambda f: lambda i, s: f(i, s) + (0,)
    pack_spec = lambda f: pl.BlockSpec((1, pack_rows, HEAD_DIM), f)
    mat_spec = lambda n, f: pl.BlockSpec((1, n, HEAD_DIM, HEAD_DIM), four(f))
    pack_shape = jax.ShapeDtypeStruct((2, pack_rows, HEAD_DIM), F32)
    mat_shape = lambda n: jax.ShapeDtypeStruct((2, n, HEAD_DIM, HEAD_DIM), F32)

    s1, k1, s2, k2, dsa, dka, dsb, dkb = pl.pallas_call(
        functools.partial(gram_kernel, per, first_part),
        grid_spec=pltpu.PrefetchScalarGridSpec(
            num_scalar_prefetch=1,
            grid=(4,),
            in_specs=[
                pl.BlockSpec((rows, block), mine),
                pl.BlockSpec((rows, block), half),
                pl.BlockSpec((rows, block), mine),
                pl.BlockSpec((rows, cut), half),
                pl.BlockSpec((rows, narrow), half),
            ],
            out_specs=[
                pack_spec(send_a),
                pack_spec(keep_a),
                pack_spec(send_b),
                pack_spec(keep_b),
                mat_spec(first_part, send_a),
                mat_spec(first_part, keep_a),
                mat_spec(rest, send_b),
                mat_spec(rest, keep_b),
            ],
        ),
        out_shape=[pack_shape] * 4 + [mat_shape(first_part)] * 2 + [mat_shape(rest)] * 2,
        name="gram",
    )(idx, x1, x1r, x2, x2ra, x2rb)

    def halve(send, keep, b_first, b_second):
        got = swap(send, b_first)
        second = swap(keep[1] + got[1], b_second)
        return keep[0] + got[0] + second

    def everyone(x):
        for b in range(4, bits):
            x = x + swap(x, b)
        return x

    gram_a = halve(s1, k1, 1, 2)
    gram_b = halve(s2, k2, 2, 1)
    low = bit[3] == 0
    keep_g = everyone(jnp.where(low, gram_a, gram_b))
    away_g = everyone(jnp.where(low, gram_b, gram_a))
    got_g = swap(away_g, 3)

    mine_w = pl.pallas_call(
        functools.partial(newton_kernel, per, tokens),
        out_shape=jax.ShapeDtypeStruct((pack_rows, HEAD_DIM), F32),
        name="newton",
    )(keep_g, got_g)

    other_w = swap(mine_w, 3)
    o01 = swap(mine_w, 2)
    o10 = swap(mine_w, 1)
    o11 = swap(o01, 1)
    e10 = swap(other_w, 1)
    e01 = swap(other_w, 2)
    e11 = swap(e10, 2)
    w1 = jnp.where(low, mine_w, other_w)
    w2 = jnp.where(low, other_w, mine_w)
    w2x = over_lay(w2, 0)

    def spread(parts, which, alias):
        theirs = [swap(p, 0) for p in parts]
        sources = list(parts) + theirs
        n = len(parts)

        def place(i, s):
            core = s[0] ^ (i // n)
            slot = i % n
            return (s[3], 0, core * quarter + (s[1] ^ (slot // 2)) * 2 + (s[2] ^ (slot % 2)), 0, 0)

        args = [jnp.stack([bit[0], bit[1], bit[2], which]).astype(jnp.int32)] + sources
        in_specs = [pl.BlockSpec((pack_rows, HEAD_DIM), lambda i, s: (0, 0)) for _ in sources]
        aliases = {}
        if alias is not None:
            aliases = {len(args): 0}
            args.append(alias)
            in_specs.append(pl.BlockSpec(memory_space=pl.ANY))
        return pl.pallas_call(
            functools.partial(spread_kernel, per, len(sources), alias is None),
            grid_spec=pltpu.PrefetchScalarGridSpec(
                num_scalar_prefetch=1,
                grid=(len(sources),),
                in_specs=in_specs,
                out_specs=pl.BlockSpec((1, 1, per, HEAD_DIM, HEAD_DIM), place),
                scratch_shapes=[pltpu.VMEM((pack_rows, HEAD_DIM), F32)],
            ),
            out_shape=jax.ShapeDtypeStruct((2, 1, heads, HEAD_DIM, HEAD_DIM), F32),
            input_output_aliases=aliases,
            name="spread",
        )(*args)

    whitening = spread([mine_w, o01, o10, o11], bit[3], None)
    whitening = spread([other_w, e01, e10, e11], 1 - bit[3], whitening)

    def finish(send_a, keep_a, send_b, keep_b, right, column):
        a = everyone(halve(send_a, keep_a, 1, 2))
        b = everyone(halve(send_b, keep_b, 2, 1))
        ca = jnp.stack([a, one_way(a, 3, 0)])
        cb = jnp.stack([b, one_way(b, 3, 1)])
        where = jnp.stack([bit[3], column, group * per]).astype(jnp.int32)
        return pl.pallas_call(
            functools.partial(similar_kernel, per, first_part, tokens),
            in_specs=[pl.BlockSpec(memory_space=pltpu.SMEM)]
            + [pl.BlockSpec(memory_space=pltpu.VMEM)] * 4,
            out_specs=pl.BlockSpec(memory_space=pltpu.VMEM),
            out_shape=jax.ShapeDtypeStruct((8, HEAD_DIM), F32),
            name="similar",
        )(where, w1, right, ca, cb)

    tile = finish(dsa, dka, dsb, dkb, w2, lay)

    def cross(lo, count, by_first, xm, xt):
        send, keep = (send_a, keep_a) if by_first else (send_b, keep_b)
        return pl.pallas_call(
            functools.partial(cross_kernel, lo, count, by_first),
            grid_spec=pltpu.PrefetchScalarGridSpec(
                num_scalar_prefetch=1,
                grid=(4,),
                in_specs=[
                    pl.BlockSpec((rows, block), mine),
                    pl.BlockSpec((rows, block), half),
                    pl.BlockSpec((rows, count * HEAD_DIM), half),
                    pl.BlockSpec((rows, count * HEAD_DIM), half),
                ],
                out_specs=[mat_spec(count, send), mat_spec(count, keep)],
            ),
            out_shape=[mat_shape(count)] * 2,
            name="cross",
        )(idx, x1, x1r, xm, xt)

    csa, cka = cross(0, first_part, True, xam, xat)
    csb, ckb = cross(first_part, rest, False, xbm, xbt)
    tile = tile + finish(csa, cka, csb, ckb, w2x, 1 - lay)
    for b in range(4):
        tile = tile + swap(tile, b)
    return whitening, tile[:2, :heads][None]


def solution(mesh):
    in_specs = (P("lay", "tok", None), P("lay", "tok", None))
    out_specs = (P(None, "lay", None, None, None), P("lay", None, None))
    return jax.shard_map(local, mesh=mesh, in_specs=in_specs, out_specs=out_specs, check_vma=False)
```

```python
import functools

import jax
import jax.numpy as jnp
from jax import lax
from jax.experimental import pallas as pl
from jax.experimental.pallas import tpu as pltpu
from jax.sharding import PartitionSpec as P


HEAD_DIM = 128
HALF = HEAD_DIM // 2
ITERS = 6
VMEM_LIMIT = 14 << 20
GROUPS = 8
RIDGE = 0.05
TOP = lax.Precision.HIGHEST
F32 = jnp.float32


def iotas(rows):
    row = lax.broadcasted_iota(jnp.int32, (rows, HEAD_DIM), 0)
    lane = lax.broadcasted_iota(jnp.int32, (rows, HEAD_DIM), 1)
    return row, lane


def pack_sym(mat):
    row, lane = iotas(HALF)
    low = mat[HALF:]
    packed = jnp.where(row <= lane, mat[:HALF], pltpu.roll(low, HALF, 1))
    diag = jnp.sum(jnp.where(lane - HALF == row, low, 0.0), axis=0, keepdims=True)
    return packed, diag


def unpack_sym(packed, diag):
    row, lane = iotas(HALF)
    square = jnp.concatenate([packed, packed], axis=0).T
    turned = square[:HALF]
    top = jnp.where(row <= lane, packed, turned)
    corner = jnp.where(row > lane - HALF, pltpu.roll(packed, HALF, 1), turned)
    corner = jnp.where(row == lane - HALF, diag, corner)
    bottom = jnp.where(lane < HALF, square[HALF:], corner)
    return jnp.concatenate([top, bottom], axis=0)


def outer(left_row, right_row):
    column = jnp.broadcast_to(left_row, (HEAD_DIM, HEAD_DIM)).T
    return column * right_row


def mm(a, b):
    return jnp.dot(a, b, precision=TOP, preferred_element_type=F32)


def contract_tokens(a, b):
    return lax.dot_general(a, b, (((0,), (0,)), ((), ())), preferred_element_type=F32)


def gram_kernel(per, idx, x1, x1r, x2, x2r, s1, k1, s2, k2, sd, kd):
    slot = pl.program_id(0)
    rows = per * HALF
    packs = [[], []]
    sums = [[], []]
    diags = [[], []]
    cross = []
    for q in range(per):
        cols = slice(q * HEAD_DIM, (q + 1) * HEAD_DIM)
        mine = jnp.concatenate([x1[:, cols], x2[:, cols]], axis=1)
        theirs = jnp.concatenate([x1r[:, cols], x2r[:, cols]], axis=1)
        both = jnp.concatenate([mine, theirs], axis=0)
        g = contract_tokens(both, both)
        total = jnp.sum(both.astype(F32), axis=0, keepdims=True)
        for c in range(2):
            part = slice(c * HEAD_DIM, (c + 1) * HEAD_DIM)
            packed, diag = pack_sym(g[part, part])
            packs[c].append(packed)
            diags[c].append(diag)
            sums[c].append(total[:, part])
        cross.append(g[:HEAD_DIM, HEAD_DIM:])

    def write(ref, c):
        for q in range(per):
            ref[0, q * HALF : (q + 1) * HALF, :] = packs[c][q]
        tail = jnp.zeros((ref.shape[1] - rows - 2 * per, HEAD_DIM), F32)
        ref[0, rows:, :] = jnp.concatenate(sums[c] + diags[c] + [tail], axis=0)

    def write_cross(ref):
        for q in range(per):
            ref[0, q] = cross[q]

    @pl.when(slot >= 2)
    def _():
        write(s1, 0)
        write_cross(sd)

    @pl.when(slot < 2)
    def _():
        write(k1, 0)
        write_cross(kd)

    @pl.when(slot % 2 == 1)
    def _():
        write(s2, 1)

    @pl.when(slot % 2 == 0)
    def _():
        write(k2, 1)


def cross_kernel(lo, count, by_first, idx, x1, x1r, xm, xt, send, keep):
    slot = pl.program_id(0)
    out = []
    for q in range(count):
        left = slice((lo + q) * HEAD_DIM, (lo + q + 1) * HEAD_DIM)
        right = slice(q * HEAD_DIM, (q + 1) * HEAD_DIM)
        a = jnp.concatenate([x1[:, left], x1r[:, left]], axis=0)
        b = jnp.concatenate([xm[:, right], xt[:, right]], axis=0)
        out.append(contract_tokens(a, b))
    moves = slot >= 2 if by_first else slot % 2 == 1

    @pl.when(moves)
    def _():
        for q in range(count):
            send[0, q] = out[q]

    @pl.when(jnp.logical_not(moves))
    def _():
        for q in range(count):
            keep[0, q] = out[q]


def newton_kernel(per, tokens, keep, recv, out):
    rows = per * HALF
    total = keep[...] + recv[...]
    row = lax.broadcasted_iota(jnp.int32, (HEAD_DIM, HEAD_DIM), 0)
    lane = lax.broadcasted_iota(jnp.int32, (HEAD_DIM, HEAD_DIM), 1)
    eye = jnp.where(row == lane, 1.0, 0.0).astype(F32)
    ys, zs, scales, means = [], [], [], []
    for q in range(per):
        gram = unpack_sym(
            total[q * HALF : (q + 1) * HALF], total[rows + per + q : rows + per + q + 1]
        )
        mean = total[rows + q : rows + q + 1] / tokens
        cov = gram / tokens - outer(mean, mean) + RIDGE * eye
        scale = jnp.sqrt(jnp.sum(cov * cov, keepdims=True))
        y = cov / scale
        ys.append(y)
        scales.append(scale)
        means.append(mean)
    fs = [1.5 * eye - 0.5 * y for y in ys]
    ys = [mm(y, f) for y, f in zip(ys, fs)]
    zs = fs
    for sweep in range(1, ITERS):
        fs = [1.5 * eye - 0.5 * mm(z, y) for z, y in zip(zs, ys)]
        if sweep < ITERS - 1:
            ys = [mm(y, f) for y, f in zip(ys, fs)]
        zs = [mm(f, z) for f, z in zip(fs, zs)]
    diags = []
    for q in range(per):
        packed, diag = pack_sym(zs[q] / jnp.sqrt(scales[q]))
        out[q * HALF : (q + 1) * HALF, :] = packed
        diags.append(diag)
    tail = jnp.zeros((out.shape[0] - rows - 2 * per, HEAD_DIM), F32)
    out[rows:, :] = jnp.concatenate(means + diags + [tail], axis=0)


def head_of(pack, per, q):
    rows = per * HALF
    mat = unpack_sym(pack[q * HALF : (q + 1) * HALF], pack[rows + per + q : rows + per + q + 1])
    return mat, pack[rows + q : rows + q + 1]


def whitened_square(left_head, right_head, cross, tokens):
    left, mean_left = left_head
    right, mean_right = right_head
    cross = cross / tokens - outer(mean_left, mean_right)
    white = mm(mm(left, cross), right)
    return jnp.sum(white * white, keepdims=True) / HEAD_DIM


def similar_kernel(per, entries, tokens, idx, w1, w2, w2x, mine, got, out):
    row, lane = iotas(8)
    tile = jnp.zeros((8, HEAD_DIM), F32)
    for e, (low, high) in enumerate(entries):
        cross = mine[e] + got[e]

        def pick(kind, q):
            return head_of(w1, per, q), head_of(w2x if kind else w2, per, q)

        if low == high:
            left, right = pick(*low)
            line, head = idx[1 + low[0]], low[1]
        else:
            left, right = jax.tree.map(
                lambda a, b: jnp.where(idx[0] == 0, a, b), pick(*low), pick(*high)
            )
            line = jnp.where(idx[0] == 0, idx[1 + low[0]], idx[1 + high[0]])
            head = jnp.where(idx[0] == 0, low[1], high[1])
        value = whitened_square(left, right, cross, tokens)
        tile = jnp.where((row == line) & (lane == idx[3] + head), value, tile)
    out[...] = tile


def spread_kernel(per, count, idx, *refs):
    sources = refs[:count]
    out, buf = refs[-2], refs[-1]
    step = pl.program_id(0)
    for i, source in enumerate(sources):

        @pl.when(step == i)
        def _(source=source):
            buf[: source.shape[0], :] = source[...]

    row, lane = iotas(HALF)
    rows = per * HALF

    def write(q, packed, turned, moved, low_left, diag):
        top = jnp.where(row <= lane, packed, turned)
        corner = jnp.where(row > lane - HALF, pltpu.roll(packed, HALF, 1), moved)
        corner = jnp.where(row == lane - HALF, diag, corner)
        out[0, 0, q, :HALF, :] = top
        out[0, 0, q, HALF:, :] = jnp.where(lane < HALF, low_left, corner)

    for q in range(0, per, 2):
        two = buf[q * HALF : (q + 2) * HALF, :]
        square = two.T
        rolled = pltpu.roll(square, HALF, 1)
        diag = rows + per + q
        write(q, two[:HALF], square[:HALF], rolled[:HALF], square[HALF:], buf[diag : diag + 1, :])
        if q + 1 < per:
            diag += 1
            write(
                q + 1, two[HALF:], rolled[:HALF], square[:HALF], rolled[HALF:], buf[diag : diag + 1, :]
            )


def local(first_acts, second_acts):
    n_tok = lax.axis_size("tok")
    n_lay = lax.axis_size("lay")
    layers, rows, width = first_acts.shape
    heads = width // HEAD_DIM
    bits = n_tok.bit_length() - 1
    assert layers == 1 and n_lay == 2
    assert n_tok == 1 << bits and bits >= 4 and heads % GROUPS == 0
    per = heads // GROUPS
    part_a = (per + 1) // 2
    part_b = per - part_a
    block = per * HEAD_DIM
    tokens = float(rows * n_tok)
    pack_rows = -(-(per * HALF + 2 * per) // 8) * 8

    tok = lax.axis_index("tok")
    lay = lax.axis_index("lay")
    bit = [(tok >> b) & 1 for b in range(bits)]

    def swap(x, b):
        return lax.ppermute(x, "tok", [(i, i ^ (1 << b)) for i in range(n_tok)])

    def over_lay(x):
        return lax.ppermute(x, "lay", [(0, 1), (1, 0)])

    def everyone(x):
        for b in range(4, bits):
            x = x + swap(x, b)
        return x

    def call(kernel, *args, **options):
        params = pltpu.CompilerParams(vmem_limit_bytes=VMEM_LIMIT)
        return pl.pallas_call(kernel, compiler_params=params, **options)(*args)

    x1 = first_acts[0]
    x2 = second_acts[0]
    quarter = GROUPS // 2
    group = bit[0] * quarter + bit[1] * 2 + bit[2]
    idx = jnp.stack([bit[0], bit[1], bit[2], bit[3], 1 - bit[3]]).astype(jnp.int32)
    bf = first_acts.dtype

    x1r = swap(x1, 0)
    x2r = swap(x2, 0)

    def pack(lo, count):
        size = count * HEAD_DIM

        def body(src, out, sem):
            copies = [
                pltpu.make_async_copy(
                    src.at[:, g * block + lo * HEAD_DIM : g * block + lo * HEAD_DIM + size],
                    out.at[:, g * size : (g + 1) * size],
                    sem.at[g],
                )
                for g in range(GROUPS)
            ]
            for copy in copies:
                copy.start()
            for copy in copies:
                copy.wait()

        return call(
            body,
            x2,
            in_specs=[pl.BlockSpec(memory_space=pl.ANY)],
            out_specs=pl.BlockSpec(memory_space=pl.ANY),
            out_shape=jax.ShapeDtypeStruct((rows, GROUPS * size), bf),
            scratch_shapes=[pltpu.SemaphoreType.DMA((GROUPS,))],
        )

    xa = over_lay(pack(0, part_a))
    xb = over_lay(pack(part_a, part_b))

    def mine(i, s):
        return (0, s[0] * quarter + (s[1] ^ (i // 2)) * 2 + (s[2] ^ (i % 2)))

    send_a = lambda i, s: (jnp.maximum(i - 2, 0), 0, 0)
    keep_a = lambda i, s: (jnp.minimum(i, 1), 0, 0)
    send_b = lambda i, s: (i // 3, 0, 0)
    keep_b = lambda i, s: (i // 2, 0, 0)
    four = lambda f: lambda i, s: f(i, s) + (0,)
    pack_spec = lambda f: pl.BlockSpec((1, pack_rows, HEAD_DIM), f)
    mat_spec = lambda n, f: pl.BlockSpec((1, n, HEAD_DIM, HEAD_DIM), four(f))
    pack_shape = jax.ShapeDtypeStruct((2, pack_rows, HEAD_DIM), F32)
    mat_shape = lambda n: jax.ShapeDtypeStruct((2, n, HEAD_DIM, HEAD_DIM), F32)

    s1, k1, s2, k2, sd, kd = call(
        functools.partial(gram_kernel, per),
        idx,
        x1,
        x1r,
        x2,
        x2r,
        grid_spec=pltpu.PrefetchScalarGridSpec(
            num_scalar_prefetch=1,
            grid=(4,),
            in_specs=[pl.BlockSpec((rows, block), mine)] * 4,
            out_specs=[
                pack_spec(send_a),
                pack_spec(keep_a),
                pack_spec(send_b),
                pack_spec(keep_b),
                mat_spec(per, send_a),
                mat_spec(per, keep_a),
            ],
        ),
        out_shape=[pack_shape] * 4 + [mat_shape(per)] * 2,
    )

    def halve(send, keep, b_first, b_second, after=None):
        got = swap(send, b_first)
        if after is not None:
            got, _ = lax.optimization_barrier((got, after))
        second = swap(keep[1] + got[1], b_second)
        return everyone(keep[0] + got[0] + second)

    low = bit[3] == 0
    gram_a = halve(s1, k1, 1, 2)
    gram_b = halve(s2, k2, 2, 1)
    keep_g = jnp.where(low, gram_a, gram_b)
    got_g = swap(jnp.where(low, gram_b, gram_a), 3)

    own_w = call(
        functools.partial(newton_kernel, per, tokens),
        keep_g,
        got_g,
        out_shape=jax.ShapeDtypeStruct((pack_rows, HEAD_DIM), F32),
    )

    diag = halve(sd, kd, 1, 2, own_w)

    other_w = swap(own_w, 3)
    o01 = swap(own_w, 2)
    o10 = swap(own_w, 1)
    o11 = swap(o01, 1)
    e10 = swap(other_w, 1)
    e01 = swap(other_w, 2)
    e11 = swap(e10, 2)
    w1 = jnp.where(low, own_w, other_w)
    w2 = jnp.where(low, other_w, own_w)
    w2x = over_lay(w2)

    def spread(parts, which, alias):
        theirs = [swap(p, 0) for p in parts]
        sources = list(parts) + theirs
        n = len(parts)

        def place(i, s):
            core = s[0] ^ (i // n)
            slot = i % n
            return (
                s[which],
                0,
                core * quarter + (s[1] ^ (slot // 2)) * 2 + (s[2] ^ (slot % 2)),
                0,
                0,
            )

        args = [idx] + sources
        in_specs = [pl.BlockSpec((pack_rows, HEAD_DIM), lambda i, s: (0, 0)) for _ in sources]
        aliases = {}
        if alias is not None:
            aliases = {len(args): 0}
            args.append(alias)
            in_specs.append(pl.BlockSpec(memory_space=pl.ANY))
        return call(
            functools.partial(spread_kernel, per, len(sources)),
            *args,
            grid_spec=pltpu.PrefetchScalarGridSpec(
                num_scalar_prefetch=1,
                grid=(len(sources),),
                in_specs=in_specs,
                out_specs=pl.BlockSpec((1, 1, per, HEAD_DIM, HEAD_DIM), place),
                scratch_shapes=[pltpu.VMEM((max(pack_rows, -(-per // 2) * HEAD_DIM), HEAD_DIM), F32)],
            ),
            out_shape=jax.ShapeDtypeStruct((2, 1, heads, HEAD_DIM, HEAD_DIM), F32),
            input_output_aliases=aliases,
        )

    whitening = spread([own_w, o01, o10, o11], 3, None)
    whitening = spread([other_w, e01, e10, e11], 4, whitening)

    def cross(lo, count, by_first, xm, xt):
        send, keep = (send_a, keep_a) if by_first else (send_b, keep_b)
        return call(
            functools.partial(cross_kernel, lo, count, by_first),
            idx,
            x1,
            x1r,
            xm,
            xt,
            grid_spec=pltpu.PrefetchScalarGridSpec(
                num_scalar_prefetch=1,
                grid=(4,),
                in_specs=[pl.BlockSpec((rows, block), mine)] * 2
                + [pl.BlockSpec((rows, count * HEAD_DIM), mine)] * 2,
                out_specs=[mat_spec(count, send), mat_spec(count, keep)],
            ),
            out_shape=[mat_shape(count)] * 2,
        )

    where = jnp.stack([bit[3], lay, 1 - lay, group * per]).astype(jnp.int32)

    def similar(entries, kept, got):
        return call(
            functools.partial(similar_kernel, per, entries, tokens),
            where,
            w1,
            w2,
            w2x,
            kept,
            got,
            in_specs=[pl.BlockSpec(memory_space=pltpu.SMEM)]
            + [pl.BlockSpec(memory_space=pltpu.VMEM)] * 5,
            out_specs=pl.BlockSpec(memory_space=pltpu.VMEM),
            out_shape=jax.ShapeDtypeStruct((8, HEAD_DIM), F32),
        )

    csa, cka = cross(0, part_a, True, xa, swap(xa, 0))
    cross_a = halve(csa, cka, 1, 2)
    jobs = [(0, q) for q in range(per)] + [(1, q) for q in range(part_a)]
    half = (len(jobs) + 1) // 2
    early = jnp.concatenate([diag, cross_a], axis=0)
    first_half, second_half = early[:half], early[len(jobs) - half :]
    got_a = swap(jnp.where(low, second_half, first_half), 3)
    kept_a = jnp.where(low, first_half, second_half)
    entries = list(zip(jobs[:half], jobs[len(jobs) - half :]))
    tile_a = similar(entries, kept_a, got_a)
    if len(jobs) % 2:
        line = jnp.where(lay == 0, jobs[half - 1][0], 1 - jobs[half - 1][0])
        spot = jnp.arange(8)[:, None] == line
        spot &= jnp.arange(HEAD_DIM)[None] == group * per + jobs[half - 1][1]
        tile_a = jnp.where(spot & jnp.logical_not(low), 0.0, tile_a)
    tile_a = tile_a + swap(tile_a, 3)

    csb, ckb = cross(part_a, part_b, False, xb, swap(xb, 0))
    cross_b = halve(csb, ckb, 2, 1)
    got_b = swap(cross_b, 3)
    jobs_b = [(1, part_a + q) for q in range(part_b)]
    tile = tile_a + similar(list(zip(jobs_b, jobs_b)), cross_b, got_b)
    for b in (2, 1, 0):
        tile = tile + swap(tile, b)
    return whitening, tile[:2, :heads][None]


def solution(mesh):
    in_specs = (P("lay", "tok", None), P("lay", "tok", None))
    out_specs = (P(None, "lay", None, None, None), P("lay", None, None))

    return jax.shard_map(local, mesh=mesh, in_specs=in_specs, out_specs=out_specs, check_vma=False)
```
